32 devices in a mesh: slab: 8 (over y, x, core), atom: 4 (over z).
Axes of the slice: x: 2, y: 2, z: 4, core: 2. Of those that a mesh axis runs over, the one named last changes fastest.
Arguments:
- cells: int32 [3, 512, 512], P(None, 'slab', 'atom'), may hold values from 0 to 255, as said below
- fractions: float32 [3, 512, 512], P(None, 'slab', 'atom'), may hold values from 0 to 1
- charges: float32 [512, 512], P('slab', 'atom'), may hold values from -3 to 3
- counts: int32 [512, 4], P('slab', 'atom'), may hold values from 1 to 128, as said below
- box: float32 [3], replicated, may hold values from 192 to 243.2
Outputs:
- kfield: float32 [2, 256, 256, 256], P(None, 'slab', 'atom')
- totals: float32 [7], replicated
The draws below stay inside these ranges and needn't reach their ends.
Inputs may be any that keep to these rules, and one draw needn't show every extreme that they name: `cells`: for row r (tile r mod 64 of slab r div 64) every slot's z cell lies in the 32 planes from (r div 64) * 32 and its y cell in the 4 rows from (r mod 64) * 4; x anywhere. `counts`: live slots are the first ones of a tile's 128; some tile is full in every draw.
All inputs are finite; a program needn't handle non-finite values.
Results may differ from the reference program's by a relative error of at most 0.000078.
Values sent between devices are 32-bit elements; how exact they have to be, the bound alone decides.
No kernel may reach another device: no remote copies, remote signals or barrier semaphores. Data moves between devices by JAX's collectives and lax.ppermute only.
A program may use at most 192 MiB of HBM per device.

```python
import math
import jax
import jax.numpy as jnp
from jax import lax

K = 256
TILES = 64
SLOTS = 128
DZ = 32
TY = 4
ROWS = 512
COLS = 512


def draw_cells(key, part):
    keys = jax.random.split(jax.random.fold_in(key, 11), 3)
    row_ids = jnp.arange(ROWS, dtype=jnp.int32)[:, None]
    zcell = row_ids // TILES * DZ + jax.random.randint(keys[0], (ROWS, COLS), 0, DZ)
    ycell = row_ids % TILES * TY + jax.random.randint(keys[1], (ROWS, COLS), 0, TY)
    xcell = jax.random.randint(keys[2], (ROWS, COLS), 0, K)
    return jnp.stack([zcell, ycell, xcell]).astype(jnp.int32)


def draw_counts(key, part):
    first, second = jax.random.split(jax.random.fold_in(key, 23))
    shards = COLS // SLOTS
    filled = jax.random.randint(first, (ROWS * shards,), 1, SLOTS + 1)
    where = jax.random.randint(second, (), 0, ROWS * shards)
    filled = filled.at[where].set(SLOTS)
    return filled.reshape(ROWS, shards).astype(jnp.int32)


def block_levels(stream_key, shape, cuts, smallest, top_value):
    factor_of = 1.0
    for axis_at, parts in cuts:
        heights = jax.random.uniform(jax.random.fold_in(jax.random.fold_in(stream_key, 6), axis_at), (parts,), jnp.float32, smallest / len(cuts), top_value / len(cuts))
        factor_of = factor_of * jnp.repeat(jnp.exp(heights), shape[axis_at] // parts).reshape((-1,) + (1,) * (len(shape) - 1 - axis_at))
    return factor_of


def scatter_about(key, extent, spread, most, cuts=(), kind=jnp.bfloat16):
    loudness = block_levels(key, extent, cuts, -0.22, 0.18) if cuts else 1.0
    entries = jax.random.normal(key, extent, jnp.float32) * spread * loudness
    return jnp.minimum(jnp.maximum(entries, -most), most).astype(kind)


def setup_inputs(seed: int = 0) -> dict:
    arg_keys = jax.random.split(jax.random.key(seed), 6)
    cells = draw_cells(jax.random.fold_in(arg_keys[5], 71), 0)
    fractions = jnp.clip(1.0 * jax.random.uniform(arg_keys[1], (3, ROWS, COLS), jnp.float32) ** block_levels(arg_keys[1], (3, ROWS, COLS), ((1, 8), (2, 4)), -0.2, 0.2), 0.0, 1.0)
    charges = scatter_about(arg_keys[2], (ROWS, COLS), 0.5, 3.0, ((0, 8), (1, 4)), jnp.float32)
    counts = draw_counts(jax.random.fold_in(arg_keys[5], 71), 0)
    box = jnp.clip(jax.random.uniform(arg_keys[4], (3,), jnp.float32, 192.0, 243.2), 192.0, 243.2)
    return dict(cells=cells, fractions=fractions, charges=charges, counts=counts, box=box)


ewald_beta = 1.25


def spline_weights(frac):
    prior = [jnp.ones_like(frac)]
    for order in range(2, 7):
        nxt = []
        for i in range(order):
            point = frac + i
            here = prior[i] if i < order - 1 else jnp.zeros_like(frac)
            lower = prior[i - 1] if i > 0 else jnp.zeros_like(frac)
            nxt.append((point * here + (order - point) * lower) / (order - 1))
        prior = nxt
    return prior


def moduli(index):
    angle = (index % K).astype(jnp.float32) * (2.0 * math.pi / K)
    denom = 66.0 + 52.0 * jnp.cos(angle) + 2.0 * jnp.cos(2.0 * angle)
    return (120.0 / denom) ** 2


def reference(cells, fractions, charges, counts, box):
    rows, cols = charges.shape
    column = jnp.arange(cols, dtype=jnp.int32)
    limit = counts[:, column // SLOTS]
    live = ((column % SLOTS)[None, :] < limit).astype(jnp.float32)
    weight = charges * live
    along_z = jnp.stack(spline_weights(fractions[0]))
    along_y = jnp.stack(spline_weights(fractions[1]))
    along_x = spline_weights(fractions[2])

    def add_pair(pair, flat):
        first = pair // 6
        second = pair % 6
        zcell = (cells[0] + 3 - first) % K
        ycell = (cells[1] + 3 - second) % K
        base = weight * along_z[first] * along_y[second]
        for third in range(6):
            xcell = (cells[2] + 3 - third) % K
            flat = flat.at[(zcell * K + ycell) * K + xcell].add(base * along_x[third])
        return flat

    flat = lax.fori_loop(0, 36, add_pair, jnp.zeros((K * K * K,), jnp.float32))
    spectrum = jnp.fft.fftn(flat.reshape(K, K, K))
    real_part = jnp.transpose(jnp.real(spectrum), (1, 2, 0)).astype(jnp.float32)
    imag_part = jnp.transpose(jnp.imag(spectrum), (1, 2, 0)).astype(jnp.float32)
    index = jnp.arange(K, dtype=jnp.int32)
    folded = jnp.where(index < K // 2, index, index - K).astype(jnp.float32)
    m_z = (folded / box[0])[None, None, :]
    m_y = (folded / box[1])[:, None, None]
    m_x = (folded / box[2])[None, :, None]
    msq = m_z * m_z + m_y * m_y + m_x * m_x
    anchor = (index[:, None, None] == 0) & (index[None, :, None] == 0) & (index[None, None, :] == 0)
    safe = jnp.where(anchor, 1.0, msq)
    volume = box[0] * box[1] * box[2]
    spline_part = moduli(index)[None, None, :] * moduli(index)[:, None, None] * moduli(index)[None, :, None]
    theta = jnp.exp(-(math.pi ** 2) * safe / ewald_beta ** 2) * spline_part / (math.pi * volume * safe)
    theta = jnp.where(anchor, 0.0, theta)
    kfield = jnp.stack([theta * real_part, theta * imag_part])
    half = 0.5 * theta * (real_part * real_part + imag_part * imag_part)
    factor = 2.0 * (1.0 + (math.pi ** 2) * safe / ewald_beta ** 2) / safe
    count = rows * cols
    totals = jnp.stack([
        jnp.sum(half),
        jnp.sum(half * (1.0 - factor * m_z * m_z)),
        jnp.sum(half * (1.0 - factor * m_y * m_y)),
        jnp.sum(half * (1.0 - factor * m_x * m_x)),
        jnp.sum(half * (-factor * m_z * m_y)),
        jnp.sum(half * (-factor * m_z * m_x)),
        jnp.sum(half * (-factor * m_y * m_x)),
    ]) / count
    return kfield, totals
```

```python
import functools
import math

import jax
import jax.numpy as jnp
import numpy as np
from jax import lax
from jax.experimental import pallas as pl
from jax.experimental.pallas import tpu as pltpu
from jax.sharding import PartitionSpec as P

K = 256
TILES = 64
ORDER = 6
BELOW = 2
ABOVE = 3
HALO = BELOW + ABOVE

ewald_beta = 1.25
f32 = jnp.float32
bf16 = jnp.bfloat16


def split_const(table):
    high = np.asarray(table, np.float32).astype(jnp.bfloat16)
    low = (np.asarray(table, np.float64) - high.astype(np.float64)).astype(np.float32)
    return high, low.astype(jnp.bfloat16)


def dft_const():
    index = np.arange(K)
    angle = 2.0 * np.pi * (np.outer(index, index) % K) / K
    return np.cos(angle), np.sin(angle)


def moduli_const():
    angle = 2.0 * np.pi * np.arange(K) / K
    denom = 66.0 + 52.0 * np.cos(angle) + 2.0 * np.cos(2.0 * angle)
    return ((120.0 / denom) ** 2).astype(np.float32)


def split(x):
    high = x.astype(bf16)
    low = (x - high.astype(f32)).astype(bf16)
    return high, low


def dot(a, b):
    return lax.dot_general(a, b, (((1,), (0,)), ((), ())), preferred_element_type=f32)


def dot_nt(a, b):
    return lax.dot_general(a, b, (((1,), (1,)), ((), ())), preferred_element_type=f32)


def spline_taps(frac):
    prior = [jnp.ones_like(frac)]
    for order in range(2, ORDER + 1):
        scale = 1.0 / (order - 1)
        nxt = []
        for i in range(order):
            terms = []
            if i < order - 1:
                terms.append(((frac + i) * scale) * prior[i])
            if i > 0:
                terms.append(((order - i) - frac) * scale * prior[i - 1])
            nxt.append(terms[0] if len(terms) == 1 else terms[0] + terms[1])
        prior = nxt
    return prior


def iota(shape, dim):
    return lax.broadcasted_iota(jnp.int32, shape, dim)


def spread_kernel(
    counts, where_x, atoms, table_x, high_y, low_y, out, left, right, packed, *, shards, tiles, slots, depth, rows_tile
):
    planes = depth + HALO
    stride = -(-planes // 8) * 8
    window = rows_tile + HALO
    fields = 7 * tiles + 8
    group = 2 * slots
    quarter = table_x.shape[2] // 2

    left[...] = jnp.zeros_like(left)
    right[...] = jnp.zeros_like(right)

    def tile_step(t, _):
        lanes = iota((1, slots), 1)
        sums = [jnp.zeros((7, slots), f32) for _ in range(shards)]
        offset = jnp.int32(0)
        for j in range(shards):
            count = counts[j, t]
            rows = jnp.concatenate(
                [atoms[pl.ds(j * fields + f * tiles + t, 1), :] for f in range(7)], axis=0
            )
            rolled = pltpu.roll(rows, offset & (slots - 1), 1)
            for g in range(j + 1):
                at = lanes + g * slots
                sums[g] = jnp.where((at >= offset) & (at < offset + count), rolled, sums[g])
            offset = offset + count
        for g in range(shards):
            packed[pl.ds(0, 7), pl.ds(g * slots, slots)] = sums[g]

        def group_step(k, _):
            part = packed[:, pl.ds(pl.multiple_of(k * group, group), group)]
            taps = spline_taps(part)
            cell = part.astype(jnp.int32)
            weight = part[6:7]

            def row_of(i, r):
                return taps[i][r : r + 1]

            from_z = iota((stride, group), 0) - (cell[0:1] & (depth - 1))
            along_z = jnp.zeros((stride, group), f32)
            from_y = iota((16, group), 0) - (cell[1:2] & (rows_tile - 1))
            along_y = jnp.zeros((16, group), f32)
            start = (cell[2:3] - BELOW) & (K - 1)
            lane_s = iota((8, group), 0)
            within = start & 7
            turn = (lane_s - within) & 7
            block = ((start >> 3) + jnp.where(lane_s < within, 1, 0)) & (K // 8 - 1)
            along_x = jnp.zeros((8, group), f32)
            for i in range(ORDER):
                hit = ORDER - 1 - i
                along_z = jnp.where(from_z == hit, row_of(i, 3) * weight, along_z)
                along_y = jnp.where(from_y == hit, row_of(i, 4), along_y)
                along_x = jnp.where(turn == hit, row_of(i, 5), along_x)
            x_high = along_x.astype(bf16).astype(f32)
            x_low = along_x - x_high
            highs, lows = [], []
            for b in range(K // 8):
                mask = block == b
                highs.append(jnp.where(mask, x_high, 0.0))
                lows.append(jnp.where(mask, x_low, 0.0))
            t_high = jnp.concatenate(highs, axis=0).astype(bf16)
            t_low = jnp.concatenate(lows, axis=0).astype(bf16)
            outer = jnp.concatenate(
                [along_z * along_y[q : q + 1] for q in range(window)]
                + [jnp.zeros((8, group), f32)] * (window * stride % 16 // 8),
                axis=0,
            )
            o_high, o_low = split(outer)
            result = dot_nt(o_high, t_high) + dot_nt(o_high, t_low) + dot_nt(o_low, t_high)
            at = pl.ds(pl.multiple_of(t * (rows_tile * stride), 8), window * stride)
            left[at, :] += result[: window * stride, : K // 2]
            right[at, :] += result[: window * stride, K // 2 :]
            return 0

        lax.fori_loop(0, (offset + group - 1) // group, group_step, 0)
        return 0

    packed[...] = jnp.zeros_like(packed)
    lax.fori_loop(0, tiles, tile_step, 0)
    for ref in (left, right):
        ref[pl.ds(K * stride, BELOW * stride), :] += ref[pl.ds(0, BELOW * stride), :]
        ref[pl.ds(BELOW * stride, ABOVE * stride), :] += ref[pl.ds((K + BELOW) * stride, ABOVE * stride), :]

    sign = jnp.where(iota((1, 2 * (quarter // 2)), 1) < quarter // 2, 1.0, -1.0)

    def plane_step(p, _):
        at = pl.ds(BELOW * stride + p, K, stride=stride)
        plane = jnp.concatenate([left[at, :], right[at, :]], axis=1)
        high, low = split(plane)
        tab = table_x[where_x[0]]
        first = dot(high, tab)
        in_x = first[:, :quarter] + first[:, quarter:] + dot(low, tab[:, :quarter])
        xh, xl = split(in_x)
        second = dot(high_y[...], jnp.concatenate([xh, xl], axis=1))
        in_y = second[:, :quarter] + second[:, quarter:] + dot(low_y[...], xh)
        by_cos, by_sin = in_y[:K], in_y[K:]
        done = by_cos + pltpu.roll(by_sin, quarter // 2, 1) * sign
        slot = jnp.where(p < BELOW, p + ABOVE + depth, p + ABOVE - BELOW)
        slot = jnp.where(p < BELOW + depth, slot, p - BELOW - depth)
        out[pl.ds(slot, K, stride=planes), :] = done
        return 0

    lax.fori_loop(0, planes, plane_step, 0)


def final_kernel(
    where_k, box, data, table_high, table_low, mod_row, mod_col, field, sums, m_y, g_y, acc, *, slabs, depth, quarter, n_dev, norm
):
    planes = depth + HALO
    pair = 2
    scale = math.pi**2 / ewald_beta**2

    def folded(index):
        return jnp.where(index < K // 2, index, index - K).astype(f32)

    row_z = folded(iota((1, K), 1)) / box[0]
    col_x = folded(iota((quarter, 1), 0) + where_k[1] * quarter) / box[2]
    rows_y = folded(iota((depth, K), 0) + where_k[0] * depth) / box[1]
    mod_x = mod_col[pl.ds(pl.multiple_of(where_k[1] * quarter, 8), quarter), :]
    mod_y = mod_col[pl.ds(pl.multiple_of(where_k[0] * depth, 8), depth), :]
    m_y[...] = rows_y
    g_y[...] = jnp.exp(-scale * rows_y * rows_y) * mod_y
    volume = box[0] * box[1] * box[2]
    base_zx = jnp.exp(-scale * row_z * row_z) * mod_row[...] * (
        jnp.exp(-scale * col_x * col_x) * mod_x / (math.pi * volume)
    )
    sq_zx = row_z * row_z + col_x * col_x
    acc[...] = jnp.zeros_like(acc)
    ids = iota((8, 2 * quarter), 0)

    def step(k, _):
        tr = []
        for u in range(pair):
            ky = k * pair + u
            blocks = []
            for s in range(slabs):
                here = (s * depth + ky) * planes
                before = (((s - 1) % slabs) * depth + ky) * planes
                after = (((s + 1) % slabs) * depth + ky) * planes
                first = data[pl.ds(here + ABOVE, 8), :] + jnp.where(
                    ids < ABOVE, data[pl.ds(before, 8), :], 0.0
                )
                mid = data[pl.ds(here + ABOVE + 8, depth - 16), :]
                last = data[pl.ds(here + ABOVE + depth - 8, 8), :] + jnp.where(
                    ids >= 8 - BELOW, data[pl.ds(after + planes - 8, 8), :], 0.0
                )
                blocks += [first, mid, last]
            tr.append(jnp.concatenate(blocks, axis=0).T)
        high, low = split(jnp.concatenate(tr, axis=0))
        both = dot(high, table_high[...]) + dot(high, table_low[...]) + dot(low, table_high[...])
        for u in range(pair):
            ky = k * pair + u
            lo, mi, hi = (2 * u * quarter, (2 * u + 1) * quarter, (2 * u + 2) * quarter)
            real = both[lo:mi, :K] + both[mi:hi, K:]
            imag = both[mi:hi, :K] - both[lo:mi, K:]
            my = m_y[pl.ds(ky, 1), :]
            msq = sq_zx + my * my
            anchor = msq == 0.0
            inverse = 1.0 / jnp.where(anchor, 1.0, msq)
            theta = jnp.where(anchor, 0.0, base_zx * g_y[pl.ds(ky, 1), :] * inverse)
            fr = theta * real
            fi = theta * imag
            field[0, ky] = fr
            field[1, ky] = fi
            half = 0.5 * (fr * real + fi * imag)
            g = half * (2.0 * inverse + 2.0 * scale)
            gy = g * my
            acc[0] += half
            acc[1] += g
            acc[2] += gy
            acc[3] += gy * my
        return 0

    lax.fori_loop(0, depth // pair, step, 0)

    def total(x):
        return jnp.sum(jnp.sum(x, axis=0, keepdims=True), axis=1, keepdims=True)

    energy = total(acc[0])
    g, gy = acc[1], acc[2]
    values = [
        energy,
        energy - total(g * row_z * row_z),
        energy - total(acc[3]),
        energy - total(g * col_x * col_x),
        -total(gy * row_z),
        -total(g * row_z * col_x),
        -total(gy * col_x),
    ]
    lane = iota((n_dev, 128), 1)
    line = jnp.zeros((n_dev, 128), f32)
    for i, value in enumerate(values):
        line = jnp.where(lane == i, value * norm, line)
    sums[...] = line


def vmem():
    return pl.BlockSpec(memory_space=pltpu.VMEM)


def smem():
    return pl.BlockSpec(memory_space=pltpu.SMEM)


def body(cells, fractions, charges, counts, box):
    slabs = lax.axis_size("slab")
    shards = lax.axis_size("atom")
    tiles, slots = charges.shape
    depth = K // slabs
    quarter = K // shards
    rows_tile = K // tiles
    planes = depth + HALO
    stride = -(-planes // 8) * 8
    n_dev = slabs * shards
    norm = 1.0 / (tiles * slabs * slots * shards)
    a = lax.axis_index("atom").astype(jnp.int32)
    s = lax.axis_index("slab").astype(jnp.int32)

    live = (jnp.arange(slots, dtype=jnp.int32)[None, :] < counts).astype(f32)
    mine = jnp.concatenate(
        [
            cells.astype(f32).reshape(3 * tiles, slots),
            fractions.reshape(3 * tiles, slots),
            charges * live,
            jnp.broadcast_to(jnp.pad(counts[:, 0].astype(f32), (0, slots - tiles))[None], (8, slots)),
        ]
    )
    gathered = lax.all_gather(mine, "atom", axis=0)
    all_counts = gathered[:, 7 * tiles, :tiles].astype(jnp.int32)

    cosine, sine = dft_const()
    per_x = []
    for i in range(shards):
        part = slice(i * quarter, (i + 1) * quarter)
        high, low = split_const(np.concatenate([cosine[:, part], -sine[:, part]], axis=1))
        per_x.append(np.concatenate([high, low], axis=1))
    table_x = jnp.asarray(np.stack(per_x))
    high_y, low_y = split_const(np.concatenate([cosine, sine], axis=0))
    high_z, low_z = split_const(np.concatenate([cosine, sine], axis=1))

    fields = 7 * tiles + 8
    spectrum = pl.pallas_call(
        functools.partial(
            spread_kernel, shards=shards, tiles=tiles, slots=slots, depth=depth, rows_tile=rows_tile
        ),
        out_shape=jax.ShapeDtypeStruct((K * planes, 2 * quarter), f32),
        in_specs=[smem(), smem(), vmem(), vmem(), vmem(), vmem()],
        out_specs=vmem(),
        scratch_shapes=[
            pltpu.VMEM(((K + HALO) * stride, K // 2), f32),
            pltpu.VMEM(((K + HALO) * stride, K // 2), f32),
            pltpu.VMEM((8, shards * slots), f32),
        ],
        compiler_params=pltpu.CompilerParams(vmem_limit_bytes=60 * 1024 * 1024),
        name="spread",
    )(
        all_counts,
        a[None],
        gathered.reshape(shards * fields, slots),
        table_x,
        jnp.asarray(high_y),
        jnp.asarray(low_y),
    )
    moved = lax.all_to_all(
        spectrum.reshape(slabs, depth * planes, 2 * quarter), "slab", 0, 0, tiled=True
    )
    mod = moduli_const()
    if depth % 16:
        return plain_final(moved, box, high_z, a, s, slabs, depth, quarter, norm)
    field, sums = pl.pallas_call(
        functools.partial(
            final_kernel, slabs=slabs, depth=depth, quarter=quarter, n_dev=n_dev, norm=norm
        ),
        out_shape=(
            jax.ShapeDtypeStruct((2, depth, quarter, K), f32),
            jax.ShapeDtypeStruct((n_dev, 128), f32),
        ),
        in_specs=[smem(), smem(), vmem(), vmem(), vmem(), vmem(), vmem()],
        out_specs=(vmem(), vmem()),
        scratch_shapes=[
            pltpu.VMEM((depth, K), f32),
            pltpu.VMEM((depth, K), f32),
            pltpu.VMEM((4, quarter, K), f32),
        ],
        compiler_params=pltpu.CompilerParams(vmem_limit_bytes=60 * 1024 * 1024),
        name="final",
    )(
        jnp.stack([s, a]),
        box,
        moved.reshape(K * planes, 2 * quarter),
        jnp.asarray(high_z),
        jnp.asarray(low_z),
        jnp.asarray(mod[None, :]),
        jnp.asarray(mod[:, None]),
    )
    return field, spread_totals(sums)


def spread_totals(sums):
    shared = lax.all_to_all(sums, ("slab", "atom"), 0, 0, tiled=True)
    return jnp.sum(shared[:, :7], axis=0)


def plain_final(moved, box, table, a, s, slabs, depth, quarter, norm):
    planes = depth + HALO
    highest = lax.Precision.HIGHEST
    data = moved.reshape(slabs, depth, planes, 2 * quarter)
    own = data[:, :, ABOVE : ABOVE + depth]
    up = jnp.roll(data[:, :, :ABOVE], 1, axis=0)
    down = jnp.roll(data[:, :, ABOVE + depth :], -1, axis=0)
    own = own.at[:, :, :ABOVE].add(up).at[:, :, depth - BELOW :].add(down)
    cosine, sine = (jnp.asarray(t.astype(np.float32)) for t in dft_const())
    flat = jnp.transpose(own, (1, 3, 0, 2)).reshape(depth, 2 * quarter, K)
    real_in, imag_in = flat[:, :quarter], flat[:, quarter:]
    times = functools.partial(jnp.einsum, "yxz,zk->yxk", precision=highest)
    real_part = times(real_in, cosine) + times(imag_in, sine)
    imag_part = times(imag_in, cosine) - times(real_in, sine)
    index_z = jnp.arange(K, dtype=jnp.int32)
    index_y = s * depth + jnp.arange(depth, dtype=jnp.int32)
    index_x = a * quarter + jnp.arange(quarter, dtype=jnp.int32)
    mod = jnp.asarray(moduli_const())

    def folded(index):
        return jnp.where(index < K // 2, index, index - K).astype(f32)

    m_z = (folded(index_z) / box[0])[None, None, :]
    m_y = (folded(index_y) / box[1])[:, None, None]
    m_x = (folded(index_x) / box[2])[None, :, None]
    msq = m_z * m_z + m_y * m_y + m_x * m_x
    anchor = msq == 0.0
    safe = jnp.where(anchor, 1.0, msq)
    volume = box[0] * box[1] * box[2]
    spline_part = mod[index_z][None, None, :] * mod[index_y][:, None, None] * mod[index_x][None, :, None]
    theta = jnp.exp(-math.pi**2 * safe / ewald_beta**2) * spline_part / (math.pi * volume * safe)
    theta = jnp.where(anchor, 0.0, theta)
    half = 0.5 * theta * (real_part * real_part + imag_part * imag_part)
    factor = 2.0 * (1.0 + math.pi**2 * safe / ewald_beta**2) / safe
    terms = [
        half,
        half * (1.0 - factor * m_z * m_z),
        half * (1.0 - factor * m_y * m_y),
        half * (1.0 - factor * m_x * m_x),
        half * (-factor * m_z * m_y),
        half * (-factor * m_z * m_x),
        half * (-factor * m_y * m_x),
    ]
    totals = lax.psum(jnp.stack([jnp.sum(term) for term in terms]), ("slab", "atom")) * norm
    return jnp.stack([theta * real_part, theta * imag_part]), totals


def solution(mesh):
    in_specs = (
        P(None, "slab", "atom"),
        P(None, "slab", "atom"),
        P("slab", "atom"),
        P("slab", "atom"),
        P(),
    )
    out_specs = (P(None, "slab", "atom", None), P())
    return jax.shard_map(body, mesh=mesh, in_specs=in_specs, out_specs=out_specs, check_vma=False)
```

```python
import functools
import math

import jax
import jax.numpy as jnp
import numpy as np
from jax import lax
from jax.experimental import pallas as pl
from jax.experimental.pallas import tpu as pltpu
from jax.sharding import PartitionSpec as P

K = 256
TILES = 64
ORDER = 6
BELOW = 2
ABOVE = 3
HALO = BELOW + ABOVE

ewald_beta = 1.25
f32 = jnp.float32
bf16 = jnp.bfloat16


def split_const(table):
    high = np.asarray(table, np.float32).astype(jnp.bfloat16)
    low = (np.asarray(table, np.float64) - high.astype(np.float64)).astype(np.float32)
    return high, low.astype(jnp.bfloat16)


def dft_const():
    index = np.arange(K)
    angle = 2.0 * np.pi * (np.outer(index, index) % K) / K
    return np.cos(angle), np.sin(angle)


def moduli_const():
    angle = 2.0 * np.pi * np.arange(K) / K
    denom = 66.0 + 52.0 * np.cos(angle) + 2.0 * np.cos(2.0 * angle)
    return ((120.0 / denom) ** 2).astype(np.float32)


def split(x):
    high = x.astype(bf16)
    low = (x - high.astype(f32)).astype(bf16)
    return high, low


def dot(a, b):
    return lax.dot_general(a, b, (((1,), (0,)), ((), ())), preferred_element_type=f32)


def dot_nt(a, b):
    return lax.dot_general(a, b, (((1,), (1,)), ((), ())), preferred_element_type=f32)


def spline_taps(frac):
    ups = [frac] + [frac + float(i) for i in range(1, ORDER - 1)]
    downs = [None] + [float(i) - frac for i in range(1, ORDER)]
    prior = [jnp.ones_like(frac)]
    for order in range(2, ORDER + 1):
        nxt = []
        for i in range(order):
            if i == 0:
                nxt.append(ups[0] * prior[0])
            elif i == order - 1:
                nxt.append(downs[1] * prior[i - 1])
            else:
                nxt.append(ups[i] * prior[i] + downs[order - i] * prior[i - 1])
        prior = nxt
    return prior


def iota(shape, dim):
    return lax.broadcasted_iota(jnp.int32, shape, dim)


def join_kernel(cells, fractions, charges, counts, out, *, tiles):
    out[pl.ds(0, 3 * tiles), :] = cells[...].astype(f32)
    out[pl.ds(3 * tiles, 3 * tiles), :] = fractions[...]
    out[pl.ds(6 * tiles, tiles), :] = charges[...]
    out[pl.ds(7 * tiles, 8), :] = jnp.zeros((8, out.shape[1]), f32)
    out[pl.ds(7 * tiles, 1), pl.ds(0, tiles)] = counts[...].astype(f32)


def pack_tiles(counts, atoms, packed, items, clear, *, shards, tiles, slots):
    fields = 7 * tiles + 8
    most = shards // 2
    lanes = iota((1, slots), 1)
    zero = jnp.zeros((7, slots), f32)

    def step(t, n):
        clear(t)
        sums = [zero] * shards
        offset = jnp.int32(0)
        for j in range(shards):
            count = counts[j, t]
            rows = atoms[pl.ds(j * fields + t, 7, stride=tiles), :]
            rolled = pltpu.roll(rows, offset & (slots - 1), 1)
            for g in range(j + 1):
                at = lanes + g * slots
                sums[g] = jnp.where((at >= offset) & (at < offset + count), rolled, sums[g])
            offset = offset + count
        for g in range(most):
            both = jnp.concatenate([sums[2 * g], sums[2 * g + 1]], axis=1)
            packed[pl.ds(pl.multiple_of((t * most + g) * 8, 8), 8), :] = jnp.concatenate(
                [both, jnp.zeros((1, 2 * slots), f32)], axis=0
            )
            items[n + g] = t * most + g
        return n + (offset + 2 * slots - 1) // (2 * slots)

    n = lax.fori_loop(0, tiles, step, jnp.int32(0))
    packed[pl.ds(tiles * most * 8, 8), :] = jnp.zeros((8, 2 * slots), f32)
    for g in range(2):
        items[n + g] = tiles * most
    return n


def build_tables(part, left_table, right_table, *, stride, window, depth, rows_tile, group):
    taps = spline_taps(part)
    cell = part.astype(jnp.int32)
    weight = part[6:7] * (1.0 / math.factorial(ORDER - 1) ** 3)

    def row_of(i, r):
        return taps[i][r : r + 1]

    start_z = cell[0:1] & (depth - 1)
    start_x = (cell[2:3] - BELOW) & (K - 1)
    id_z, id_x = iota((8, group), 0), iota((16, group), 0)
    within_z, within_x = start_z & 7, start_x & 15
    turn_z, turn_x = (id_z - within_z) & 7, (id_x - within_x) & 15
    block_z = (start_z >> 3) + jnp.where(id_z < within_z, 1, 0)
    block_x = ((start_x >> 4) + jnp.where(id_x < within_x, 1, 0)) & (K // 16 - 1)
    from_y = iota((16, group), 0) - (cell[1:2] & (rows_tile - 1))
    some_z = jnp.zeros((8, group), f32)
    some_x = jnp.zeros((16, group), f32)
    along_y = jnp.zeros((16, group), f32)
    for i in range(ORDER):
        hit = ORDER - 1 - i
        some_z = jnp.where(turn_z == hit, row_of(i, 3) * weight, some_z)
        along_y = jnp.where(from_y == hit, row_of(i, 4), along_y)
        some_x = jnp.where(turn_x == hit, row_of(i, 5), some_x)
    along_z = jnp.concatenate([jnp.where(block_z == b, some_z, 0.0) for b in range(stride // 8)], axis=0)
    x_high, x_low = split(some_x)
    block = block_x.astype(f32).astype(bf16)
    none = jnp.zeros((16, group), bf16)
    for b in range(K // 16):
        mask = block == jnp.asarray(b, bf16)
        right_table[pl.ds(b * 16, 16), pl.ds(0, group)] = jnp.where(mask, x_high, none)
        right_table[pl.ds(b * 16, 16), pl.ds(group, group)] = jnp.where(mask, x_low, none)
    for q in range(0, window, 2):
        rows = [along_z * along_y[u : u + 1] for u in range(q, min(q + 2, window))]
        height = len(rows) * stride
        if height % 16:
            rows.append(jnp.zeros((8, group), f32))
            height += 8
        high, low = split(jnp.concatenate(rows, axis=0))
        left_table[pl.ds(q * stride, height), pl.ds(0, group)] = high
        left_table[pl.ds(q * stride, height), pl.ds(group, group)] = low


def spread_kernel(
    counts,
    where_x,
    atoms,
    table_x,
    high_y,
    low_y,
    out,
    left,
    right,
    packed,
    items,
    lt_a,
    rt_a,
    lt_b,
    rt_b,
    *,
    shards,
    tiles,
    slots,
    depth,
    rows_tile,
):
    planes = depth + HALO
    stride = -(-planes // 8) * 8
    window = rows_tile + HALO
    group = 2 * slots
    most = shards // 2
    half = table_x.shape[2] // 2
    quarter = half // 2
    step_rows = rows_tile * stride

    def clear(t):
        for ref in (left, right):
            ref[pl.ds(pl.multiple_of(t * step_rows, 8), step_rows), :] = jnp.zeros((step_rows, K // 2), f32)

    for ref in (left, right):
        ref[pl.ds(K * stride, HALO * stride), :] = jnp.zeros((HALO * stride, K // 2), f32)
    count = pack_tiles(counts, atoms, packed, items, clear, shards=shards, tiles=tiles, slots=slots)

    def build(i, lt, rt):
        part = packed[pl.ds(pl.multiple_of(items[i] * 8, 8), 8), :]
        build_tables(
            part, lt, rt, stride=stride, window=window, depth=depth, rows_tile=rows_tile, group=group
        )

    def apply(i, lt, rt):
        t = jnp.minimum(items[i] // most, tiles - 1)
        lh, ll = lt[:, :group], lt[:, group:]
        rh, rl = rt[:, :group], rt[:, group:]
        result = dot_nt(
            jnp.concatenate([lh, lh, ll], axis=1), jnp.concatenate([rh, rl, rh], axis=1)
        )
        at = pl.ds(pl.multiple_of(t * step_rows, 8), window * stride)
        left[at, :] += result[: window * stride, : K // 2]
        right[at, :] += result[: window * stride, K // 2 :]

    build(0, lt_a, rt_a)

    def pair_step(j, _):
        apply(2 * j, lt_a, rt_a)
        build(2 * j + 1, lt_b, rt_b)
        apply(2 * j + 1, lt_b, rt_b)
        build(jnp.minimum(2 * j + 2, count), lt_a, rt_a)
        return 0

    lax.fori_loop(0, (count + 1) // 2, pair_step, 0)
    for ref in (left, right):
        ref[pl.ds(K * stride, BELOW * stride), :] += ref[pl.ds(0, BELOW * stride), :]
        ref[pl.ds(BELOW * stride, ABOVE * stride), :] += ref[pl.ds((K + BELOW) * stride, ABOVE * stride), :]

    chunk = 512
    table = table_x[where_x[0]]

    def x_step(c, _):
        at = pl.ds(pl.multiple_of(BELOW * stride + c * chunk, 8), chunk)
        high, low = split(jnp.concatenate([left[at, :], right[at, :]], axis=1))
        upper = dot(high, table)
        lower = dot(low, table[:, :half])
        left[at, :] = (upper[:, :half] + lower) + upper[:, half:]
        return 0

    lax.fori_loop(0, K * stride // chunk, x_step, 0)

    sign = jnp.where(iota((1, half), 1) < quarter, 1.0, -1.0)
    th, tl = high_y[...], low_y[...]

    def slot_of(p):
        slot = jnp.where(p < BELOW, p + ABOVE + depth, p + ABOVE - BELOW)
        return jnp.where(p < BELOW + depth, slot, p - BELOW - depth)

    table_y = jnp.concatenate([th[:K], th[K:], th[:K], th[K:], tl[:K], tl[K:]], axis=1)

    def plane_pair(first):
        at = [first, first + 1]
        data = [left[pl.ds(BELOW * stride + p, K, stride=stride), :] for p in at]
        turned = [pltpu.roll(x, quarter, 1) * sign for x in data]
        high, low = split(jnp.concatenate(data, axis=1))
        high_t, low_t = split(jnp.concatenate(turned, axis=1))
        done = dot(table_y, jnp.concatenate([high, high_t, low, low_t, high, high_t], axis=0))
        for u in range(2):
            out[pl.ds(slot_of(at[u]), K, stride=planes), :] = done[:, u * half : (u + 1) * half]

    def plane_step(j, _):
        for u in range(2):
            plane_pair(jnp.minimum(4 * j + 2 * u, planes - 2))
        return 0

    lax.fori_loop(0, -(-planes // 4), plane_step, 0)


def final_kernel(
    where_k, box, data, table_high, table_low, mod_row, mod_col, field, sums, m_y, g_y, acc, base_zx, sq_zx, *, slabs, depth, quarter, n_dev, norm
):
    planes = depth + HALO
    pair = 4
    here_y = m_y.shape[0]
    g = pl.program_id(0)
    scale = math.pi**2 / ewald_beta**2

    def folded(index):
        return jnp.where(index < K // 2, index, index - K).astype(f32)

    row_z = folded(iota((1, K), 1)) / box[0]
    col_x = folded(iota((quarter, 1), 0) + where_k[1] * quarter) / box[2]

    @pl.when(g == 0)
    def _():
        mod_x = mod_col[pl.ds(pl.multiple_of(where_k[1] * quarter, 8), quarter), :]
        volume = box[0] * box[1] * box[2]
        base_zx[...] = jnp.exp(-scale * row_z * row_z) * mod_row[...] * (
            jnp.exp(-scale * col_x * col_x) * mod_x / (math.pi * volume)
        )
        sq_zx[...] = row_z * row_z + col_x * col_x
        acc[...] = jnp.zeros_like(acc)

    first_y = where_k[0] * depth + g * here_y
    rows_y = folded(iota((here_y, K), 0) + first_y) / box[1]
    m_y[...] = rows_y
    g_y[...] = jnp.exp(-scale * rows_y * rows_y) * mod_col[pl.ds(pl.multiple_of(first_y, 8), here_y), :]
    ids = iota((8, 2 * quarter), 0)

    def step(k, _):
        tr = []
        for u in range(pair):
            row = (k * pair + u) * planes
            blocks = []
            for s in range(slabs):
                first = data[s, pl.ds(row + ABOVE, 8), :] + jnp.where(
                    ids < ABOVE, data[(s - 1) % slabs, pl.ds(row, 8), :], 0.0
                )
                mid = data[s, pl.ds(row + ABOVE + 8, depth - 16), :]
                last = data[s, pl.ds(row + ABOVE + depth - 8, 8), :] + jnp.where(
                    ids >= 8 - BELOW, data[(s + 1) % slabs, pl.ds(row + planes - 8, 8), :], 0.0
                )
                blocks += [first, mid, last]
            tr.append(jnp.concatenate(blocks, axis=0).T)
        high, low = split(jnp.concatenate(tr, axis=0))
        th, tl = table_high[...], table_low[...]
        both = dot(jnp.concatenate([high, high, low], axis=1), jnp.concatenate([th, tl, th], axis=0))
        for u in range(pair):
            ky = k * pair + u
            lo, mi, hi = (2 * u * quarter, (2 * u + 1) * quarter, (2 * u + 2) * quarter)
            real = both[lo:mi, :K] + both[mi:hi, K:]
            imag = both[mi:hi, :K] - both[lo:mi, K:]
            my = m_y[pl.ds(ky, 1), :]
            msq = sq_zx[...] + my * my
            anchor = msq == 0.0
            inverse = 1.0 / jnp.where(anchor, 1.0, msq)
            theta = jnp.where(anchor, 0.0, base_zx[...] * g_y[pl.ds(ky, 1), :] * inverse)
            fr = theta * real
            fi = theta * imag
            field[0, ky] = fr
            field[1, ky] = fi
            half = 0.5 * (fr * real + fi * imag)
            gain = half * (2.0 * inverse + 2.0 * scale)
            gy = gain * my
            acc[0] += half
            acc[1] += gain
            acc[2] += gy
            acc[3] += gy * my
        return 0

    lax.fori_loop(0, here_y // pair, step, 0)

    @pl.when(g == pl.num_programs(0) - 1)
    def _():
        finish(sums, acc, row_z, col_x, n_dev, norm)


def finish(sums, acc, row_z, col_x, n_dev, norm):
    def total(x):
        return jnp.sum(jnp.sum(x, axis=0, keepdims=True), axis=1, keepdims=True)

    energy = total(acc[0])
    g, gy = acc[1], acc[2]
    values = [
        energy,
        energy - total(g * row_z * row_z),
        energy - total(acc[3]),
        energy - total(g * col_x * col_x),
        -total(gy * row_z),
        -total(g * row_z * col_x),
        -total(gy * col_x),
    ]
    lane = iota((n_dev, 128), 1)
    line = jnp.zeros((n_dev, 128), f32)
    for i, value in enumerate(values):
        line = jnp.where(lane == i, value * norm, line)
    sums[...] = line


def vmem():
    return pl.BlockSpec(memory_space=pltpu.VMEM)


def smem():
    return pl.BlockSpec(memory_space=pltpu.SMEM)


def body(cells, fractions, charges, counts, box):
    slabs = lax.axis_size("slab")
    shards = lax.axis_size("atom")
    tiles, slots = charges.shape
    depth = K // slabs
    quarter = K // shards
    rows_tile = K // tiles
    planes = depth + HALO
    stride = -(-planes // 8) * 8
    n_dev = slabs * shards
    norm = 1.0 / (tiles * slabs * slots * shards)
    a = lax.axis_index("atom").astype(jnp.int32)
    s = lax.axis_index("slab").astype(jnp.int32)

    mine = pl.pallas_call(
        functools.partial(join_kernel, tiles=tiles),
        out_shape=jax.ShapeDtypeStruct((7 * tiles + 8, slots), f32),
        in_specs=[vmem()] * 4,
        out_specs=vmem(),
        name="join",
    )(
        cells.reshape(3 * tiles, slots),
        fractions.reshape(3 * tiles, slots),
        charges,
        counts.reshape(1, tiles),
    )
    gathered = lax.all_gather(mine, "atom", axis=0)
    all_counts = gathered[:, 7 * tiles, :tiles].astype(jnp.int32)

    cosine, sine = dft_const()
    per_x = []
    for i in range(shards):
        part = slice(i * quarter, (i + 1) * quarter)
        high, low = split_const(np.concatenate([cosine[:, part], -sine[:, part]], axis=1))
        per_x.append(np.concatenate([high, low], axis=1))
    table_x = jnp.asarray(np.stack(per_x))
    high_y, low_y = split_const(np.concatenate([cosine, sine], axis=0))
    high_z, low_z = split_const(np.concatenate([cosine, sine], axis=1))

    fields = 7 * tiles + 8
    spectrum = pl.pallas_call(
        functools.partial(
            spread_kernel, shards=shards, tiles=tiles, slots=slots, depth=depth, rows_tile=rows_tile
        ),
        out_shape=jax.ShapeDtypeStruct((K * planes, 2 * quarter), f32),
        in_specs=[smem(), smem(), vmem(), vmem(), vmem(), vmem()],
        out_specs=vmem(),
        scratch_shapes=[
            pltpu.VMEM(((K + HALO) * stride, K // 2), f32),
            pltpu.VMEM(((K + HALO) * stride, K // 2), f32),
            pltpu.VMEM((tiles * shards * 4 + 8, 2 * slots), f32),
            pltpu.SMEM((tiles * shards // 2 + shards,), jnp.int32),
        ]
        + [
            pltpu.VMEM((-(-(rows_tile + HALO) * stride // 16) * 16, 4 * slots), bf16),
            pltpu.VMEM((K, 4 * slots), bf16),
        ]
        * 2,
        compiler_params=pltpu.CompilerParams(vmem_limit_bytes=60 * 1024 * 1024),
        name="spread",
    )(
        all_counts,
        a[None],
        gathered.reshape(shards * fields, slots),
        table_x,
        jnp.asarray(high_y),
        jnp.asarray(low_y),
    )
    moved = lax.all_to_all(
        spectrum.reshape(slabs, depth * planes, 2 * quarter), "slab", 0, 0, tiled=True
    )
    mod = moduli_const()
    block_y = 8
    if depth % 16:
        return plain_final(moved, box, high_z, a, s, slabs, depth, quarter, norm)
    field, sums = pl.pallas_call(
        functools.partial(
            final_kernel, slabs=slabs, depth=depth, quarter=quarter, n_dev=n_dev, norm=norm
        ),
        out_shape=(
            jax.ShapeDtypeStruct((2, depth, quarter, K), f32),
            jax.ShapeDtypeStruct((n_dev, 128), f32),
        ),
        grid=(depth // block_y,),
        in_specs=[
            smem(),
            smem(),
            pl.BlockSpec((slabs, block_y * planes, 2 * quarter), lambda g: (0, g, 0)),
            vmem(),
            vmem(),
            vmem(),
            vmem(),
        ],
        out_specs=(
            pl.BlockSpec((2, block_y, quarter, K), lambda g: (0, g, 0, 0)),
            pl.BlockSpec((n_dev, 128), lambda g: (0, 0)),
        ),
        scratch_shapes=[
            pltpu.VMEM((block_y, K), f32),
            pltpu.VMEM((block_y, K), f32),
            pltpu.VMEM((4, quarter, K), f32),
            pltpu.VMEM((quarter, K), f32),
            pltpu.VMEM((quarter, K), f32),
        ],
        compiler_params=pltpu.CompilerParams(vmem_limit_bytes=60 * 1024 * 1024),
        name="final",
    )(
        jnp.stack([s, a]),
        box,
        moved,
        jnp.asarray(high_z),
        jnp.asarray(low_z),
        jnp.asarray(mod[None, :]),
        jnp.asarray(mod[:, None]),
    )
    return field, spread_totals(sums)


def spread_totals(sums):
    shared = lax.all_to_all(sums, ("slab", "atom"), 0, 0, tiled=True)
    return jnp.sum(shared[:, :7], axis=0)


def plain_final(moved, box, table, a, s, slabs, depth, quarter, norm):
    planes = depth + HALO
    highest = lax.Precision.HIGHEST
    data = moved.reshape(slabs, depth, planes, 2 * quarter)
    own = data[:, :, ABOVE : ABOVE + depth]
    up = jnp.roll(data[:, :, :ABOVE], 1, axis=0)
    down = jnp.roll(data[:, :, ABOVE + depth :], -1, axis=0)
    own = own.at[:, :, :ABOVE].add(up).at[:, :, depth - BELOW :].add(down)
    cosine, sine = (jnp.asarray(t.astype(np.float32)) for t in dft_const())
    flat = jnp.transpose(own, (1, 3, 0, 2)).reshape(depth, 2 * quarter, K)
    real_in, imag_in = flat[:, :quarter], flat[:, quarter:]
    times = functools.partial(jnp.einsum, "yxz,zk->yxk", precision=highest)
    real_part = times(real_in, cosine) + times(imag_in, sine)
    imag_part = times(imag_in, cosine) - times(real_in, sine)
    index_z = jnp.arange(K, dtype=jnp.int32)
    index_y = s * depth + jnp.arange(depth, dtype=jnp.int32)
    index_x = a * quarter + jnp.arange(quarter, dtype=jnp.int32)
    mod = jnp.asarray(moduli_const())

    def folded(index):
        return jnp.where(index < K // 2, index, index - K).astype(f32)

    m_z = (folded(index_z) / box[0])[None, None, :]
    m_y = (folded(index_y) / box[1])[:, None, None]
    m_x = (folded(index_x) / box[2])[None, :, None]
    msq = m_z * m_z + m_y * m_y + m_x * m_x
    anchor = msq == 0.0
    safe = jnp.where(anchor, 1.0, msq)
    volume = box[0] * box[1] * box[2]
    spline_part = mod[index_z][None, None, :] * mod[index_y][:, None, None] * mod[index_x][None, :, None]
    theta = jnp.exp(-math.pi**2 * safe / ewald_beta**2) * spline_part / (math.pi * volume * safe)
    theta = jnp.where(anchor, 0.0, theta)
    half = 0.5 * theta * (real_part * real_part + imag_part * imag_part)
    factor = 2.0 * (1.0 + math.pi**2 * safe / ewald_beta**2) / safe
    terms = [
        half,
        half * (1.0 - factor * m_z * m_z),
        half * (1.0 - factor * m_y * m_y),
        half * (1.0 - factor * m_x * m_x),
        half * (-factor * m_z * m_y),
        half * (-factor * m_z * m_x),
        half * (-factor * m_y * m_x),
    ]
    totals = lax.psum(jnp.stack([jnp.sum(term) for term in terms]), ("slab", "atom")) * norm
    return jnp.stack([theta * real_part, theta * imag_part]), totals


def solution(mesh):
    in_specs = (
        P(None, "slab", "atom"),
        P(None, "slab", "atom"),
        P("slab", "atom"),
        P("slab", "atom"),
        P(),
    )
    out_specs = (P(None, "slab", "atom", None), P())
    return jax.shard_map(body, mesh=mesh, in_specs=in_specs, out_specs=out_specs, check_vma=False)
```

```python
import functools
import math

import jax
import jax.numpy as jnp
import numpy as np
from jax import lax
from jax.experimental import pallas as pl
from jax.experimental.pallas import tpu as pltpu
from jax.sharding import PartitionSpec as P

K = 256
TILES = 64
ORDER = 6
BELOW = 2
ABOVE = 3
HALO = BELOW + ABOVE

ewald_beta = 1.25
f32 = jnp.float32
bf16 = jnp.bfloat16


def split_const(table):
    high = np.asarray(table, np.float32).astype(jnp.bfloat16)
    low = (np.asarray(table, np.float64) - high.astype(np.float64)).astype(np.float32)
    return high, low.astype(jnp.bfloat16)


def dft_const():
    index = np.arange(K)
    angle = 2.0 * np.pi * (np.outer(index, index) % K) / K
    return np.cos(angle), np.sin(angle)


def moduli_const():
    angle = 2.0 * np.pi * np.arange(K) / K
    denom = 66.0 + 52.0 * np.cos(angle) + 2.0 * np.cos(2.0 * angle)
    return ((120.0 / denom) ** 2).astype(np.float32)


def split(x):
    high = x.astype(bf16)
    low = (x - high.astype(f32)).astype(bf16)
    return high, low


def dot(a, b):
    return lax.dot_general(a, b, (((1,), (0,)), ((), ())), preferred_element_type=f32)


def dot_nt(a, b):
    return lax.dot_general(a, b, (((1,), (1,)), ((), ())), preferred_element_type=f32)


def spline_taps(frac):
    ups = [frac] + [frac + float(i) for i in range(1, ORDER - 1)]
    downs = [None] + [float(i) - frac for i in range(1, ORDER)]
    prior = [jnp.ones_like(frac)]
    for order in range(2, ORDER + 1):
        nxt = []
        for i in range(order):
            if i == 0:
                nxt.append(ups[0] * prior[0])
            elif i == order - 1:
                nxt.append(downs[1] * prior[i - 1])
            else:
                nxt.append(ups[i] * prior[i] + downs[order - i] * prior[i - 1])
        prior = nxt
    return prior


def iota(shape, dim):
    return lax.broadcasted_iota(jnp.int32, shape, dim)


def join_kernel(cells, fractions, charges, counts, out, *, tiles):
    out[pl.ds(0, 3 * tiles), :] = cells[...].astype(f32)
    out[pl.ds(3 * tiles, 3 * tiles), :] = fractions[...]
    out[pl.ds(6 * tiles, tiles), :] = charges[...]
    out[pl.ds(7 * tiles, 8), :] = jnp.zeros((8, out.shape[1]), f32)
    out[pl.ds(7 * tiles, 1), pl.ds(0, tiles)] = counts[...].astype(f32)


def pack_tiles(counts, atoms, packed, items, clear, *, shards, tiles, slots):
    fields = 7 * tiles + 8
    most = shards // 2
    lanes = iota((1, slots), 1)
    zero = jnp.zeros((7, slots), f32)

    def step(t, n):
        clear(t)
        sums = [zero] * shards
        offset = jnp.int32(0)
        for j in range(shards):
            count = counts[j, t]
            rows = atoms[pl.ds(j * fields + t, 7, stride=tiles), :]
            rolled = pltpu.roll(rows, offset & (slots - 1), 1)
            for g in range(j + 1):
                at = lanes + g * slots
                sums[g] = jnp.where((at >= offset) & (at < offset + count), rolled, sums[g])
            offset = offset + count
        for g in range(most):
            both = jnp.concatenate([sums[2 * g], sums[2 * g + 1]], axis=1)
            packed[pl.ds(pl.multiple_of((t * most + g) * 8, 8), 8), :] = jnp.concatenate(
                [both, jnp.zeros((1, 2 * slots), f32)], axis=0
            )
            items[n + g] = t * most + g
        return n + (offset + 2 * slots - 1) // (2 * slots)

    n = lax.fori_loop(0, tiles, step, jnp.int32(0))
    packed[pl.ds(tiles * most * 8, 8), :] = jnp.zeros((8, 2 * slots), f32)
    for g in range(6):
        items[n + g] = tiles * most
    return n


def build_right(part, right_table, factors, *, stride, depth, rows_tile, group):
    taps = spline_taps(part)
    cell = part.astype(jnp.int32)
    weight = part[6:7] * (1.0 / math.factorial(ORDER - 1) ** 3)

    def row_of(i, r):
        return taps[i][r : r + 1]

    start_z = cell[0:1] & (depth - 1)
    start_x = (cell[2:3] - BELOW) & (K - 1)
    id_z, id_x = iota((8, group), 0), iota((16, group), 0)
    within_z, within_x = start_z & 7, start_x & 15
    turn_z, turn_x = (id_z - within_z) & 7, (id_x - within_x) & 15
    block_z = (start_z >> 3) + jnp.where(id_z < within_z, 1, 0)
    block_x = ((start_x >> 4) + jnp.where(id_x < within_x, 1, 0)) & (K // 16 - 1)
    from_y = iota((16, group), 0) - (cell[1:2] & (rows_tile - 1))
    some_z = jnp.zeros((8, group), f32)
    some_x = jnp.zeros((16, group), f32)
    along_y = jnp.zeros((16, group), f32)
    for i in range(ORDER):
        hit = ORDER - 1 - i
        some_z = jnp.where(turn_z == hit, row_of(i, 3) * weight, some_z)
        along_y = jnp.where(from_y == hit, row_of(i, 4), along_y)
        some_x = jnp.where(turn_x == hit, row_of(i, 5), some_x)
    along_z = jnp.concatenate([jnp.where(block_z == b, some_z, 0.0) for b in range(stride // 8)], axis=0)
    x_high, x_low = split(some_x)
    block = block_x.astype(f32).astype(bf16)
    none = jnp.zeros((16, group), bf16)
    for b in range(K // 16):
        mask = block == jnp.asarray(b, bf16)
        right_table[pl.ds(b * 16, 16), pl.ds(0, group)] = jnp.where(mask, x_high, none)
        right_table[pl.ds(b * 16, 16), pl.ds(group, group)] = jnp.where(mask, x_low, none)
    factors[pl.ds(0, stride), :] = along_z
    factors[pl.ds(stride, 16), :] = along_y


def build_left(factors, left_table, *, stride, window, group):
    along_z = factors[pl.ds(0, stride), :]
    for q in range(0, window, 2):
        rows = [along_z * factors[pl.ds(stride + u, 1), :] for u in range(q, min(q + 2, window))]
        height = len(rows) * stride
        if height % 16:
            rows.append(jnp.zeros((8, group), f32))
            height += 8
        high, low = split(jnp.concatenate(rows, axis=0))
        left_table[pl.ds(q * stride, height), pl.ds(0, group)] = high
        left_table[pl.ds(q * stride, height), pl.ds(group, group)] = low


def spread_kernel(
    counts,
    where_x,
    atoms,
    table_x,
    high_y,
    low_y,
    out,
    grid,
    packed,
    items,
    lt_a,
    rt_a,
    et_a,
    zy_a,
    lt_b,
    rt_b,
    et_b,
    zy_b,
    yt_a,
    yt_b,
    *,
    shards,
    tiles,
    slots,
    depth,
    rows_tile,
):
    planes = depth + HALO
    stride = -(-planes // 8) * 8
    window = rows_tile + HALO
    group = 2 * slots
    most = shards // 2
    half = table_x.shape[1] // 2
    quarter = half // 2
    step_rows = rows_tile * stride
    used = window * stride
    height = lt_a.shape[0]

    def clear(t):
        grid[pl.ds(pl.multiple_of(t * step_rows, 8), step_rows), :] = jnp.zeros((step_rows, half), f32)

    grid[pl.ds(K * stride, HALO * stride), :] = jnp.zeros((HALO * stride, half), f32)
    count = pack_tiles(counts, atoms, packed, items, clear, shards=shards, tiles=tiles, slots=slots)
    phases = table_x[where_x[0]]

    def build(i, rt, zy):
        part = packed[pl.ds(pl.multiple_of(items[i] * 8, 8), 8), :]
        build_right(part, rt, zy, stride=stride, depth=depth, rows_tile=rows_tile, group=group)

    def turn(rt, zy, lt, et):
        build_left(zy, lt, stride=stride, window=window, group=group)
        upper = dot(phases, rt[:, :group])
        lower = dot(phases[:half], rt[:, group:])
        high, low = split((upper[:half] + lower) + upper[half:])
        et[pl.ds(0, half), :] = high
        et[pl.ds(half, half), :] = low

    def apply(i, lt, et):
        t = jnp.minimum(items[i] // most, tiles - 1)
        result = dot_nt(jnp.concatenate([lt[:, :group], lt[:, group:]], axis=0), et[...])
        at = pl.ds(pl.multiple_of(t * step_rows, 8), used)
        grid[at, :] += (result[:used, half:] + result[height : height + used, :half]) + result[:used, :half]

    build(0, rt_a, zy_a)
    build(1, rt_b, zy_b)
    turn(rt_a, zy_a, lt_a, et_a)
    turn(rt_b, zy_b, lt_b, et_b)
    build(2, rt_a, zy_a)
    build(3, rt_b, zy_b)

    def pair_step(j, _):
        apply(2 * j, lt_a, et_a)
        turn(rt_a, zy_a, lt_a, et_a)
        build(2 * j + 4, rt_a, zy_a)
        apply(2 * j + 1, lt_b, et_b)
        turn(rt_b, zy_b, lt_b, et_b)
        build(2 * j + 5, rt_b, zy_b)
        return 0

    lax.fori_loop(0, (count + 1) // 2, pair_step, 0)
    grid[pl.ds(K * stride, BELOW * stride), :] += grid[pl.ds(0, BELOW * stride), :]
    grid[pl.ds(BELOW * stride, ABOVE * stride), :] += grid[pl.ds((K + BELOW) * stride, ABOVE * stride), :]

    sign = jnp.where(iota((1, half), 1) < quarter, 1.0, -1.0)
    th, tl = high_y[...], low_y[...]

    def slot_of(p):
        slot = jnp.where(p < BELOW, p + ABOVE + depth, p + ABOVE - BELOW)
        return jnp.where(p < BELOW + depth, slot, p - BELOW - depth)

    table_y = jnp.concatenate([th[:K], th[K:], th[:K], th[K:], tl[:K], tl[K:]], axis=1)

    def first_of(j):
        return jnp.minimum(2 * j, planes - 2)

    def load(j, buf):
        data = [grid[pl.ds(BELOW * stride + first_of(j) + u, K, stride=stride), :] for u in range(2)]
        turned = [pltpu.roll(x, quarter, 1) * sign for x in data]
        for at, pair in ((0, data), (K, turned)):
            high, low = split(jnp.concatenate(pair, axis=1))
            buf[pl.ds(at, K), :] = high
            buf[pl.ds(at + 2 * K, K), :] = low

    def combine(j, buf):
        done = dot(table_y, jnp.concatenate([buf[...], buf[pl.ds(0, 2 * K), :]], axis=0))
        for u in range(2):
            out[pl.ds(slot_of(first_of(j) + u), K, stride=planes), :] = done[:, u * half : (u + 1) * half]

    load(0, yt_a)
    load(1, yt_b)

    def plane_step(j, _):
        combine(2 * j, yt_a)
        load(2 * j + 2, yt_a)
        combine(2 * j + 1, yt_b)
        load(2 * j + 3, yt_b)
        return 0

    lax.fori_loop(0, -(-planes // 4), plane_step, 0)


def final_kernel(
    where_k, box, data, table_high, table_low, mod_row, mod_col, field, sums, m_y, g_y, acc, base_zx, sq_zx, *, slabs, depth, quarter, n_dev, norm
):
    planes = depth + HALO
    pair = 4
    here_y = m_y.shape[0]
    g = pl.program_id(0)
    scale = math.pi**2 / ewald_beta**2

    def folded(index):
        return jnp.where(index < K // 2, index, index - K).astype(f32)

    row_z = folded(iota((1, K), 1)) / box[0]
    col_x = folded(iota((quarter, 1), 0) + where_k[1] * quarter) / box[2]

    @pl.when(g == 0)
    def _():
        mod_x = mod_col[pl.ds(pl.multiple_of(where_k[1] * quarter, 8), quarter), :]
        volume = box[0] * box[1] * box[2]
        base_zx[...] = jnp.exp(-scale * row_z * row_z) * mod_row[...] * (
            jnp.exp(-scale * col_x * col_x) * mod_x / (math.pi * volume)
        )
        sq_zx[...] = row_z * row_z + col_x * col_x
        acc[...] = jnp.zeros_like(acc)

    first_y = where_k[0] * depth + g * here_y
    rows_y = folded(iota((here_y, K), 0) + first_y) / box[1]
    m_y[...] = rows_y
    g_y[...] = jnp.exp(-scale * rows_y * rows_y) * mod_col[pl.ds(pl.multiple_of(first_y, 8), here_y), :]
    ids = iota((8, 2 * quarter), 0)

    def step(k, _):
        tr = []
        for u in range(pair):
            row = (k * pair + u) * planes
            blocks = []
            for s in range(slabs):
                first = data[s, pl.ds(row + ABOVE, 8), :] + jnp.where(
                    ids < ABOVE, data[(s - 1) % slabs, pl.ds(row, 8), :], 0.0
                )
                mid = data[s, pl.ds(row + ABOVE + 8, depth - 16), :]
                last = data[s, pl.ds(row + ABOVE + depth - 8, 8), :] + jnp.where(
                    ids >= 8 - BELOW, data[(s + 1) % slabs, pl.ds(row + planes - 8, 8), :], 0.0
                )
                blocks += [first, mid, last]
            tr.append(jnp.concatenate(blocks, axis=0).T)
        high, low = split(jnp.concatenate(tr, axis=0))
        th, tl = table_high[...], table_low[...]
        both = dot(jnp.concatenate([high, high, low], axis=1), jnp.concatenate([th, tl, th], axis=0))
        for u in range(pair):
            ky = k * pair + u
            lo, mi, hi = (2 * u * quarter, (2 * u + 1) * quarter, (2 * u + 2) * quarter)
            real = both[lo:mi, :K] + both[mi:hi, K:]
            imag = both[mi:hi, :K] - both[lo:mi, K:]
            my = m_y[pl.ds(ky, 1), :]
            msq = sq_zx[...] + my * my
            anchor = msq == 0.0
            inverse = 1.0 / jnp.where(anchor, 1.0, msq)
            theta = jnp.where(anchor, 0.0, base_zx[...] * g_y[pl.ds(ky, 1), :] * inverse)
            fr = theta * real
            fi = theta * imag
            field[0, ky] = fr
            field[1, ky] = fi
            half = 0.5 * (fr * real + fi * imag)
            gain = half * (2.0 * inverse + 2.0 * scale)
            gy = gain * my
            acc[0] += half
            acc[1] += gain
            acc[2] += gy
            acc[3] += gy * my
        return 0

    lax.fori_loop(0, here_y // pair, step, 0)

    @pl.when(g == pl.num_programs(0) - 1)
    def _():
        finish(sums, acc, row_z, col_x, n_dev, norm)


def finish(sums, acc, row_z, col_x, n_dev, norm):
    def total(x):
        return jnp.sum(jnp.sum(x, axis=0, keepdims=True), axis=1, keepdims=True)

    energy = total(acc[0])
    g, gy = acc[1], acc[2]
    values = [
        energy,
        energy - total(g * row_z * row_z),
        energy - total(acc[3]),
        energy - total(g * col_x * col_x),
        -total(gy * row_z),
        -total(g * row_z * col_x),
        -total(gy * col_x),
    ]
    lane = iota((n_dev, 128), 1)
    line = jnp.zeros((n_dev, 128), f32)
    for i, value in enumerate(values):
        line = jnp.where(lane == i, value * norm, line)
    sums[...] = line


def vmem():
    return pl.BlockSpec(memory_space=pltpu.VMEM)


def smem():
    return pl.BlockSpec(memory_space=pltpu.SMEM)


def body(cells, fractions, charges, counts, box):
    slabs = lax.axis_size("slab")
    shards = lax.axis_size("atom")
    tiles, slots = charges.shape
    depth = K // slabs
    quarter = K // shards
    rows_tile = K // tiles
    planes = depth + HALO
    stride = -(-planes // 8) * 8
    n_dev = slabs * shards
    norm = 1.0 / (tiles * slabs * slots * shards)
    a = lax.axis_index("atom").astype(jnp.int32)
    s = lax.axis_index("slab").astype(jnp.int32)

    mine = pl.pallas_call(
        functools.partial(join_kernel, tiles=tiles),
        out_shape=jax.ShapeDtypeStruct((7 * tiles + 8, slots), f32),
        in_specs=[vmem()] * 4,
        out_specs=vmem(),
        name="join",
    )(
        cells.reshape(3 * tiles, slots),
        fractions.reshape(3 * tiles, slots),
        charges,
        counts.reshape(1, tiles),
    )
    gathered = lax.all_gather(mine, "atom", axis=0)
    all_counts = gathered[:, 7 * tiles, :tiles].astype(jnp.int32)

    cosine, sine = dft_const()
    per_x = []
    for i in range(shards):
        part = slice(i * quarter, (i + 1) * quarter)
        high, low = split_const(np.concatenate([cosine[part], -sine[part]], axis=0))
        per_x.append(np.concatenate([high, low], axis=0))
    table_x = jnp.asarray(np.stack(per_x))
    high_y, low_y = split_const(np.concatenate([cosine, sine], axis=0))
    high_z, low_z = split_const(np.concatenate([cosine, sine], axis=1))

    fields = 7 * tiles + 8
    spectrum = pl.pallas_call(
        functools.partial(
            spread_kernel, shards=shards, tiles=tiles, slots=slots, depth=depth, rows_tile=rows_tile
        ),
        out_shape=jax.ShapeDtypeStruct((K * planes, 2 * quarter), f32),
        in_specs=[smem(), smem(), vmem(), vmem(), vmem(), vmem()],
        out_specs=vmem(),
        scratch_shapes=[
            pltpu.VMEM(((K + HALO) * stride, 2 * quarter), f32),
            pltpu.VMEM((tiles * shards * 4 + 8, 2 * slots), f32),
            pltpu.SMEM((tiles * shards // 2 + 8,), jnp.int32),
        ]
        + [
            pltpu.VMEM((-(-(rows_tile + HALO) * stride // 16) * 16, 4 * slots), bf16),
            pltpu.VMEM((K, 4 * slots), bf16),
            pltpu.VMEM((4 * quarter, 2 * slots), bf16),
            pltpu.VMEM((stride + 16, 2 * slots), f32),
        ]
        * 2
        + [pltpu.VMEM((4 * K, 4 * quarter), bf16)] * 2,
        compiler_params=pltpu.CompilerParams(vmem_limit_bytes=60 * 1024 * 1024),
        name="spread",
    )(
        all_counts,
        a[None],
        gathered.reshape(shards * fields, slots),
        table_x,
        jnp.asarray(high_y),
        jnp.asarray(low_y),
    )
    moved = lax.all_to_all(
        spectrum.reshape(slabs, depth * planes, 2 * quarter), "slab", 0, 0, tiled=True
    )
    mod = moduli_const()
    block_y = 8
    if depth % 16:
        return plain_final(moved, box, high_z, a, s, slabs, depth, quarter, norm)
    field, sums = pl.pallas_call(
        functools.partial(
            final_kernel, slabs=slabs, depth=depth, quarter=quarter, n_dev=n_dev, norm=norm
        ),
        out_shape=(
            jax.ShapeDtypeStruct((2, depth, quarter, K), f32),
            jax.ShapeDtypeStruct((n_dev, 128), f32),
        ),
        grid=(depth // block_y,),
        in_specs=[
            smem(),
            smem(),
            pl.BlockSpec((slabs, block_y * planes, 2 * quarter), lambda g: (0, g, 0)),
            vmem(),
            vmem(),
            vmem(),
            vmem(),
        ],
        out_specs=(
            pl.BlockSpec((2, block_y, quarter, K), lambda g: (0, g, 0, 0)),
            pl.BlockSpec((n_dev, 128), lambda g: (0, 0)),
        ),
        scratch_shapes=[
            pltpu.VMEM((block_y, K), f32),
            pltpu.VMEM((block_y, K), f32),
            pltpu.VMEM((4, quarter, K), f32),
            pltpu.VMEM((quarter, K), f32),
            pltpu.VMEM((quarter, K), f32),
        ],
        compiler_params=pltpu.CompilerParams(vmem_limit_bytes=60 * 1024 * 1024),
        name="final",
    )(
        jnp.stack([s, a]),
        box,
        moved,
        jnp.asarray(high_z),
        jnp.asarray(low_z),
        jnp.asarray(mod[None, :]),
        jnp.asarray(mod[:, None]),
    )
    return field, spread_totals(sums)


def spread_totals(sums):
    shared = lax.all_to_all(sums, ("slab", "atom"), 0, 0, tiled=True)
    return jnp.sum(shared[:, :7], axis=0)


def plain_final(moved, box, table, a, s, slabs, depth, quarter, norm):
    planes = depth + HALO
    highest = lax.Precision.HIGHEST
    data = moved.reshape(slabs, depth, planes, 2 * quarter)
    own = data[:, :, ABOVE : ABOVE + depth]
    up = jnp.roll(data[:, :, :ABOVE], 1, axis=0)
    down = jnp.roll(data[:, :, ABOVE + depth :], -1, axis=0)
    own = own.at[:, :, :ABOVE].add(up).at[:, :, depth - BELOW :].add(down)
    cosine, sine = (jnp.asarray(t.astype(np.float32)) for t in dft_const())
    flat = jnp.transpose(own, (1, 3, 0, 2)).reshape(depth, 2 * quarter, K)
    real_in, imag_in = flat[:, :quarter], flat[:, quarter:]
    times = functools.partial(jnp.einsum, "yxz,zk->yxk", precision=highest)
    real_part = times(real_in, cosine) + times(imag_in, sine)
    imag_part = times(imag_in, cosine) - times(real_in, sine)
    index_z = jnp.arange(K, dtype=jnp.int32)
    index_y = s * depth + jnp.arange(depth, dtype=jnp.int32)
    index_x = a * quarter + jnp.arange(quarter, dtype=jnp.int32)
    mod = jnp.asarray(moduli_const())

    def folded(index):
        return jnp.where(index < K // 2, index, index - K).astype(f32)

    m_z = (folded(index_z) / box[0])[None, None, :]
    m_y = (folded(index_y) / box[1])[:, None, None]
    m_x = (folded(index_x) / box[2])[None, :, None]
    msq = m_z * m_z + m_y * m_y + m_x * m_x
    anchor = msq == 0.0
    safe = jnp.where(anchor, 1.0, msq)
    volume = box[0] * box[1] * box[2]
    spline_part = mod[index_z][None, None, :] * mod[index_y][:, None, None] * mod[index_x][None, :, None]
    theta = jnp.exp(-math.pi**2 * safe / ewald_beta**2) * spline_part / (math.pi * volume * safe)
    theta = jnp.where(anchor, 0.0, theta)
    half = 0.5 * theta * (real_part * real_part + imag_part * imag_part)
    factor = 2.0 * (1.0 + math.pi**2 * safe / ewald_beta**2) / safe
    terms = [
        half,
        half * (1.0 - factor * m_z * m_z),
        half * (1.0 - factor * m_y * m_y),
        half * (1.0 - factor * m_x * m_x),
        half * (-factor * m_z * m_y),
        half * (-factor * m_z * m_x),
        half * (-factor * m_y * m_x),
    ]
    totals = lax.psum(jnp.stack([jnp.sum(term) for term in terms]), ("slab", "atom")) * norm
    return jnp.stack([theta * real_part, theta * imag_part]), totals


def solution(mesh):
    in_specs = (
        P(None, "slab", "atom"),
        P(None, "slab", "atom"),
        P("slab", "atom"),
        P("slab", "atom"),
        P(),
    )
    out_specs = (P(None, "slab", "atom", None), P())
    return jax.shard_map(body, mesh=mesh, in_specs=in_specs, out_specs=out_specs, check_vma=False)
```

```python
import functools
import math

import jax
import jax.numpy as jnp
import numpy as np
from jax import lax
from jax.experimental import pallas as pl
from jax.experimental.pallas import tpu as pltpu
from jax.sharding import PartitionSpec as P

K = 256
TILES = 64
ORDER = 6
BELOW = 2
ABOVE = 3
HALO = BELOW + ABOVE

ewald_beta = 1.25
f32 = jnp.float32
bf16 = jnp.bfloat16


def split_const(table):
    high = np.asarray(table, np.float32).astype(jnp.bfloat16)
    low = (np.asarray(table, np.float64) - high.astype(np.float64)).astype(np.float32)
    return high, low.astype(jnp.bfloat16)


def dft_const():
    index = np.arange(K)
    angle = 2.0 * np.pi * (np.outer(index, index) % K) / K
    return np.cos(angle), np.sin(angle)


def moduli_const():
    angle = 2.0 * np.pi * np.arange(K) / K
    denom = 66.0 + 52.0 * np.cos(angle) + 2.0 * np.cos(2.0 * angle)
    return ((120.0 / denom) ** 2).astype(np.float32)


def split(x):
    high = x.astype(bf16)
    low = (x - high.astype(f32)).astype(bf16)
    return high, low


def dot(a, b):
    return lax.dot_general(a, b, (((1,), (0,)), ((), ())), preferred_element_type=f32)


def dot_nt(a, b):
    return lax.dot_general(a, b, (((1,), (1,)), ((), ())), preferred_element_type=f32)


def spline_taps(frac):
    ups = [frac] + [frac + float(i) for i in range(1, ORDER - 1)]
    downs = [None] + [float(i) - frac for i in range(1, ORDER)]
    prior = [jnp.ones_like(frac)]
    for order in range(2, ORDER + 1):
        nxt = []
        for i in range(order):
            if i == 0:
                nxt.append(ups[0] * prior[0])
            elif i == order - 1:
                nxt.append(downs[1] * prior[i - 1])
            else:
                nxt.append(ups[i] * prior[i] + downs[order - i] * prior[i - 1])
        prior = nxt
    return prior


def iota(shape, dim):
    return lax.broadcasted_iota(jnp.int32, shape, dim)


def join_kernel(cells, fractions, charges, counts, out, *, tiles):
    out[pl.ds(0, 3 * tiles), :] = cells[...].astype(f32)
    out[pl.ds(3 * tiles, 3 * tiles), :] = fractions[...]
    out[pl.ds(6 * tiles, tiles), :] = charges[...]
    out[pl.ds(7 * tiles, 8), :] = jnp.zeros((8, out.shape[1]), f32)
    out[pl.ds(7 * tiles, 1), pl.ds(0, tiles)] = counts[...].astype(f32)


def pack_tiles(counts, atoms, packed, items, halves, clear, *, shards, tiles, slots):
    fields = 7 * tiles + 8
    most = shards // 2
    lanes = iota((1, slots), 1)
    zero = jnp.zeros((7, slots), f32)

    def step(t, carry):
        n, m = carry
        clear(t)
        sums = [zero] * shards
        offset = jnp.int32(0)
        for j in range(shards):
            count = counts[j, t]
            rows = atoms[pl.ds(j * fields + t, 7, stride=tiles), :]
            rolled = pltpu.roll(rows, offset & (slots - 1), 1)
            for g in range(j + 1):
                at = lanes + g * slots
                sums[g] = jnp.where((at >= offset) & (at < offset + count), rolled, sums[g])
            offset = offset + count
        for g in range(most):
            both = jnp.concatenate([sums[2 * g], sums[2 * g + 1]], axis=1)
            packed[pl.ds(pl.multiple_of((t * most + g) * 8, 8), 8), :] = jnp.concatenate(
                [both, jnp.zeros((1, 2 * slots), f32)], axis=0
            )
            items[n + g] = t * most + g
        whole = offset // (2 * slots)
        rest = offset - whole * (2 * slots)
        halves[m] = t * most + whole
        m = m + jnp.where((rest > 0) & (rest <= slots), 1, 0)
        return n + whole + jnp.where(rest > slots, 1, 0), m

    n, m = lax.fori_loop(0, tiles, step, (jnp.int32(0), jnp.int32(0)))
    packed[pl.ds(tiles * most * 8, 8), :] = jnp.zeros((8, 2 * slots), f32)
    for g in range(6):
        items[n + g] = tiles * most
        halves[m + g] = tiles * most
    return n, m


def build_right(part, right_table, factors, *, stride, depth, rows_tile, group):
    taps = spline_taps(part)
    cell = part.astype(jnp.int32)
    weight = part[6:7] * (1.0 / math.factorial(ORDER - 1) ** 3)

    def row_of(i, r):
        return taps[i][r : r + 1]

    start_z = cell[0:1] & (depth - 1)
    start_x = (cell[2:3] - BELOW) & (K - 1)
    id_z, id_x = iota((8, group), 0), iota((16, group), 0)
    within_z, within_x = start_z & 7, start_x & 15
    turn_z, turn_x = (id_z - within_z) & 7, (id_x - within_x) & 15
    block_z = (start_z >> 3) + jnp.where(id_z < within_z, 1, 0)
    block_x = ((start_x >> 4) + jnp.where(id_x < within_x, 1, 0)) & (K // 16 - 1)
    from_y = iota((16, group), 0) - (cell[1:2] & (rows_tile - 1))
    some_z = jnp.zeros((8, group), f32)
    some_x = jnp.zeros((16, group), f32)
    along_y = jnp.zeros((16, group), f32)
    for i in range(ORDER):
        hit = ORDER - 1 - i
        some_z = jnp.where(turn_z == hit, row_of(i, 3) * weight, some_z)
        along_y = jnp.where(from_y == hit, row_of(i, 4), along_y)
        some_x = jnp.where(turn_x == hit, row_of(i, 5), some_x)
    along_z = jnp.concatenate([jnp.where(block_z == b, some_z, 0.0) for b in range(stride // 8)], axis=0)
    x_high, x_low = split(some_x)
    block = block_x.astype(f32).astype(bf16)
    none = jnp.zeros((16, group), bf16)
    for b in range(K // 16):
        mask = block == jnp.asarray(b, bf16)
        right_table[pl.ds(b * 16, 16), pl.ds(0, group)] = jnp.where(mask, x_high, none)
        right_table[pl.ds(b * 16, 16), pl.ds(group, group)] = jnp.where(mask, x_low, none)
    factors[pl.ds(0, stride), :] = along_z
    factors[pl.ds(stride, 16), :] = along_y


def build_left(factors, left_table, *, stride, window, group):
    along_z = factors[pl.ds(0, stride), :]
    for q in range(0, window, 2):
        rows = [along_z * factors[pl.ds(stride + u, 1), :] for u in range(q, min(q + 2, window))]
        height = len(rows) * stride
        if height % 16:
            rows.append(jnp.zeros((8, group), f32))
            height += 8
        high, low = split(jnp.concatenate(rows, axis=0))
        left_table[pl.ds(q * stride, height), pl.ds(0, group)] = high
        left_table[pl.ds(q * stride, height), pl.ds(group, group)] = low


def spread_kernel(
    counts,
    where_x,
    atoms,
    table_x,
    high_y,
    low_y,
    out,
    grid,
    packed,
    items,
    halves,
    lt_a,
    rt_a,
    et_a,
    zy_a,
    lt_b,
    rt_b,
    et_b,
    zy_b,
    yt_a,
    yt_b,
    hlt_a,
    hrt_a,
    het_a,
    hzy_a,
    hlt_b,
    hrt_b,
    het_b,
    hzy_b,
    *,
    shards,
    tiles,
    slots,
    depth,
    rows_tile,
):
    planes = depth + HALO
    stride = -(-planes // 8) * 8
    window = rows_tile + HALO
    group = 2 * slots
    most = shards // 2
    half = table_x.shape[1] // 2
    quarter = half // 2
    step_rows = rows_tile * stride
    used = window * stride
    height = lt_a.shape[0]

    def clear(t):
        grid[pl.ds(pl.multiple_of(t * step_rows, 8), step_rows), :] = jnp.zeros((step_rows, half), f32)

    grid[pl.ds(K * stride, HALO * stride), :] = jnp.zeros((HALO * stride, half), f32)
    count, count_half = pack_tiles(counts, atoms, packed, items, halves, clear, shards=shards, tiles=tiles, slots=slots)
    phases = table_x[where_x[0]]

    def build(i, rt, zy):
        part = packed[pl.ds(pl.multiple_of(items[i] * 8, 8), 8), :]
        build_right(part, rt, zy, stride=stride, depth=depth, rows_tile=rows_tile, group=group)

    def turn(rt, zy, lt, et):
        build_left(zy, lt, stride=stride, window=window, group=group)
        upper = dot(phases, rt[:, :group])
        lower = dot(phases[:half], rt[:, group:])
        high, low = split((upper[:half] + lower) + upper[half:])
        et[pl.ds(0, half), :] = high
        et[pl.ds(half, half), :] = low

    def apply(i, lt, et):
        t = jnp.minimum(items[i] // most, tiles - 1)
        result = dot_nt(jnp.concatenate([lt[:, :group], lt[:, group:]], axis=0), et[...])
        at = pl.ds(pl.multiple_of(t * step_rows, 8), used)
        grid[at, :] += (result[:used, half:] + result[height : height + used, :half]) + result[:used, :half]

    def build_half(i, rt, zy):
        part = packed[pl.ds(pl.multiple_of(halves[i] * 8, 8), 8), pl.ds(0, slots)]
        build_right(part, rt, zy, stride=stride, depth=depth, rows_tile=rows_tile, group=slots)

    def turn_half(rt, zy, lt, et):
        build_left(zy, lt, stride=stride, window=window, group=slots)
        both = dot(phases, rt[...])
        high, low = split((both[:half, :slots] + both[:half, slots:]) + both[half:, :slots])
        et[pl.ds(0, half), pl.ds(0, slots)] = high
        et[pl.ds(0, half), pl.ds(slots, slots)] = high
        et[pl.ds(half, half), pl.ds(0, slots)] = low

    def apply_half(i, lt, et):
        t = jnp.minimum(halves[i] // most, tiles - 1)
        result = dot_nt(lt[...], et[...])
        at = pl.ds(pl.multiple_of(t * step_rows, 8), used)
        grid[at, :] += result[:used, half:] + result[:used, :half]

    def run(number, make, shift, add, first, second):
        (lt, rt, et, zy), (lt2, rt2, et2, zy2) = first, second
        make(0, rt, zy)
        make(1, rt2, zy2)
        shift(rt, zy, lt, et)
        shift(rt2, zy2, lt2, et2)
        make(2, rt, zy)
        make(3, rt2, zy2)

        def pair_step(j, _):
            add(2 * j, lt, et)
            shift(rt, zy, lt, et)
            make(2 * j + 4, rt, zy)
            add(2 * j + 1, lt2, et2)
            shift(rt2, zy2, lt2, et2)
            make(2 * j + 5, rt2, zy2)
            return 0

        lax.fori_loop(0, (number + 1) // 2, pair_step, 0)

    run(count, build, turn, apply, (lt_a, rt_a, et_a, zy_a), (lt_b, rt_b, et_b, zy_b))
    for ref in (het_a, het_b):
        ref[pl.ds(half, half), pl.ds(slots, slots)] = jnp.zeros((half, slots), bf16)
    run(
        count_half, build_half, turn_half, apply_half, (hlt_a, hrt_a, het_a, hzy_a), (hlt_b, hrt_b, het_b, hzy_b)
    )
    grid[pl.ds(K * stride, BELOW * stride), :] += grid[pl.ds(0, BELOW * stride), :]
    grid[pl.ds(BELOW * stride, ABOVE * stride), :] += grid[pl.ds((K + BELOW) * stride, ABOVE * stride), :]

    sign = jnp.where(iota((1, half), 1) < quarter, 1.0, -1.0)
    th, tl = high_y[...], low_y[...]

    def slot_of(p):
        slot = jnp.where(p < BELOW, p + ABOVE + depth, p + ABOVE - BELOW)
        return jnp.where(p < BELOW + depth, slot, p - BELOW - depth)

    table_y = jnp.concatenate([th[:K], th[K:], th[:K], th[K:], tl[:K], tl[K:]], axis=1)

    def first_of(j):
        return jnp.minimum(2 * j, planes - 2)

    def load(j, buf):
        data = [grid[pl.ds(BELOW * stride + first_of(j) + u, K, stride=stride), :] for u in range(2)]
        turned = [pltpu.roll(x, quarter, 1) * sign for x in data]
        for at, pair in ((0, data), (K, turned)):
            high, low = split(jnp.concatenate(pair, axis=1))
            buf[pl.ds(at, K), :] = high
            buf[pl.ds(at + 2 * K, K), :] = low

    def combine(j, buf):
        done = dot(table_y, jnp.concatenate([buf[...], buf[pl.ds(0, 2 * K), :]], axis=0))
        for u in range(2):
            out[pl.ds(slot_of(first_of(j) + u), K, stride=planes), :] = done[:, u * half : (u + 1) * half]

    load(0, yt_a)
    load(1, yt_b)

    def plane_step(j, _):
        combine(2 * j, yt_a)
        load(2 * j + 2, yt_a)
        combine(2 * j + 1, yt_b)
        load(2 * j + 3, yt_b)
        return 0

    lax.fori_loop(0, -(-planes // 4), plane_step, 0)


def final_kernel(
    where_k, box, data, table_high, table_low, mod_row, mod_col, field, sums, m_y, g_y, acc, base_zx, sq_zx, zt_a, zt_b, both_a, both_b, *, slabs, depth, quarter, n_dev, norm
):
    planes = depth + HALO
    pair = 4
    here_y = m_y.shape[0]
    zts, boths = (zt_a, zt_b), (both_a, both_b)
    g = pl.program_id(0)
    scale = math.pi**2 / ewald_beta**2

    def folded(index):
        return jnp.where(index < K // 2, index, index - K).astype(f32)

    row_z = folded(iota((1, K), 1)) / box[0]
    col_x = folded(iota((quarter, 1), 0) + where_k[1] * quarter) / box[2]

    @pl.when(g == 0)
    def _():
        mod_x = mod_col[pl.ds(pl.multiple_of(where_k[1] * quarter, 8), quarter), :]
        volume = box[0] * box[1] * box[2]
        base_zx[...] = jnp.exp(-scale * row_z * row_z) * mod_row[...] * (
            jnp.exp(-scale * col_x * col_x) * mod_x / (math.pi * volume)
        )
        sq_zx[...] = row_z * row_z + col_x * col_x
        acc[...] = jnp.zeros_like(acc)

    first_y = where_k[0] * depth + g * here_y
    rows_y = folded(iota((here_y, K), 0) + first_y) / box[1]
    m_y[...] = rows_y
    g_y[...] = jnp.exp(-scale * rows_y * rows_y) * mod_col[pl.ds(pl.multiple_of(first_y, 8), here_y), :]
    ids = iota((8, 2 * quarter), 0)

    def load(k, zt):
        tr = []
        for u in range(pair):
            row = (k * pair + u) * planes
            blocks = []
            for s in range(slabs):
                first = data[s, pl.ds(row + ABOVE, 8), :] + jnp.where(
                    ids < ABOVE, data[(s - 1) % slabs, pl.ds(row, 8), :], 0.0
                )
                mid = data[s, pl.ds(row + ABOVE + 8, depth - 16), :]
                last = data[s, pl.ds(row + ABOVE + depth - 8, 8), :] + jnp.where(
                    ids >= 8 - BELOW, data[(s + 1) % slabs, pl.ds(row + planes - 8, 8), :], 0.0
                )
                blocks += [first, mid, last]
            high, low = split(jnp.concatenate(blocks, axis=0).T)
            zt[pl.ds(u * 2 * quarter, 2 * quarter), pl.ds(0, K)] = high
            zt[pl.ds(u * 2 * quarter, 2 * quarter), pl.ds(K, K)] = low

    def transform(zt, both):
        th, tl = table_high[...], table_low[...]
        both[...] = dot(
            jnp.concatenate([zt[...], zt[:, :K]], axis=1), jnp.concatenate([th, th, tl], axis=0)
        )

    def weigh(k, both):
        for u in range(pair):
            ky = k * pair + u
            lo, hi = pl.ds(2 * u * quarter, quarter), pl.ds((2 * u + 1) * quarter, quarter)
            real = both[lo, :K] + both[hi, K:]
            imag = both[hi, :K] - both[lo, K:]
            my = m_y[pl.ds(ky, 1), :]
            msq = sq_zx[...] + my * my
            anchor = msq == 0.0
            inverse = 1.0 / jnp.where(anchor, 1.0, msq)
            theta = jnp.where(anchor, 0.0, base_zx[...] * g_y[pl.ds(ky, 1), :] * inverse)
            fr = theta * real
            fi = theta * imag
            field[0, ky] = fr
            field[1, ky] = fi
            half = 0.5 * (fr * real + fi * imag)
            gain = half * (2.0 * inverse + 2.0 * scale)
            gy = gain * my
            acc[0] += half
            acc[1] += gain
            acc[2] += gy
            acc[3] += gy * my

    steps = here_y // pair
    for k in range(steps + 2):
        if k >= 2:
            weigh(k - 2, boths[k % 2])
        if 1 <= k <= steps:
            transform(zts[(k - 1) % 2], boths[(k - 1) % 2])
        if k < steps:
            load(k, zts[k % 2])

    @pl.when(g == pl.num_programs(0) - 1)
    def _():
        finish(sums, acc, row_z, col_x, n_dev, norm)


def finish(sums, acc, row_z, col_x, n_dev, norm):
    def total(x):
        return jnp.sum(jnp.sum(x, axis=0, keepdims=True), axis=1, keepdims=True)

    energy = total(acc[0])
    g, gy = acc[1], acc[2]
    values = [
        energy,
        energy - total(g * row_z * row_z),
        energy - total(acc[3]),
        energy - total(g * col_x * col_x),
        -total(gy * row_z),
        -total(g * row_z * col_x),
        -total(gy * col_x),
    ]
    lane = iota((n_dev, 128), 1)
    line = jnp.zeros((n_dev, 128), f32)
    for i, value in enumerate(values):
        line = jnp.where(lane == i, value * norm, line)
    sums[...] = line


def vmem():
    return pl.BlockSpec(memory_space=pltpu.VMEM)


def smem():
    return pl.BlockSpec(memory_space=pltpu.SMEM)


def body(cells, fractions, charges, counts, box):
    slabs = lax.axis_size("slab")
    shards = lax.axis_size("atom")
    tiles, slots = charges.shape
    depth = K // slabs
    quarter = K // shards
    rows_tile = K // tiles
    planes = depth + HALO
    stride = -(-planes // 8) * 8
    n_dev = slabs * shards
    norm = 1.0 / (tiles * slabs * slots * shards)
    a = lax.axis_index("atom").astype(jnp.int32)
    s = lax.axis_index("slab").astype(jnp.int32)

    mine = pl.pallas_call(
        functools.partial(join_kernel, tiles=tiles),
        out_shape=jax.ShapeDtypeStruct((7 * tiles + 8, slots), f32),
        in_specs=[vmem()] * 4,
        out_specs=vmem(),
        name="join",
    )(
        cells.reshape(3 * tiles, slots),
        fractions.reshape(3 * tiles, slots),
        charges,
        counts.reshape(1, tiles),
    )
    gathered = lax.all_gather(mine, "atom", axis=0)
    all_counts = gathered[:, 7 * tiles, :tiles].astype(jnp.int32)

    cosine, sine = dft_const()
    per_x = []
    for i in range(shards):
        part = slice(i * quarter, (i + 1) * quarter)
        high, low = split_const(np.concatenate([cosine[part], -sine[part]], axis=0))
        per_x.append(np.concatenate([high, low], axis=0))
    table_x = jnp.asarray(np.stack(per_x))
    high_y, low_y = split_const(np.concatenate([cosine, sine], axis=0))
    high_z, low_z = split_const(np.concatenate([cosine, sine], axis=1))

    fields = 7 * tiles + 8
    spectrum = pl.pallas_call(
        functools.partial(
            spread_kernel, shards=shards, tiles=tiles, slots=slots, depth=depth, rows_tile=rows_tile
        ),
        out_shape=jax.ShapeDtypeStruct((K * planes, 2 * quarter), f32),
        in_specs=[smem(), smem(), vmem(), vmem(), vmem(), vmem()],
        out_specs=vmem(),
        scratch_shapes=[
            pltpu.VMEM(((K + HALO) * stride, 2 * quarter), f32),
            pltpu.VMEM((tiles * shards * 4 + 8, 2 * slots), f32),
            pltpu.SMEM((tiles * shards // 2 + 8,), jnp.int32),
            pltpu.SMEM((tiles + 8,), jnp.int32),
        ]
        + [
            pltpu.VMEM((-(-(rows_tile + HALO) * stride // 16) * 16, 4 * slots), bf16),
            pltpu.VMEM((K, 4 * slots), bf16),
            pltpu.VMEM((4 * quarter, 2 * slots), bf16),
            pltpu.VMEM((stride + 16, 2 * slots), f32),
        ]
        * 2
        + [pltpu.VMEM((4 * K, 4 * quarter), bf16)] * 2
        + [
            pltpu.VMEM((-(-(rows_tile + HALO) * stride // 16) * 16, 2 * slots), bf16),
            pltpu.VMEM((K, 2 * slots), bf16),
            pltpu.VMEM((4 * quarter, 2 * slots), bf16),
            pltpu.VMEM((stride + 16, slots), f32),
        ]
        * 2,
        compiler_params=pltpu.CompilerParams(vmem_limit_bytes=60 * 1024 * 1024),
        name="spread",
    )(
        all_counts,
        a[None],
        gathered.reshape(shards * fields, slots),
        table_x,
        jnp.asarray(high_y),
        jnp.asarray(low_y),
    )
    moved = lax.all_to_all(
        spectrum.reshape(slabs, depth * planes, 2 * quarter), "slab", 0, 0, tiled=True
    )
    mod = moduli_const()
    block_y = 16
    if depth % 16:
        return plain_final(moved, box, high_z, a, s, slabs, depth, quarter, norm)
    field, sums = pl.pallas_call(
        functools.partial(
            final_kernel, slabs=slabs, depth=depth, quarter=quarter, n_dev=n_dev, norm=norm
        ),
        out_shape=(
            jax.ShapeDtypeStruct((2, depth, quarter, K), f32),
            jax.ShapeDtypeStruct((n_dev, 128), f32),
        ),
        grid=(depth // block_y,),
        in_specs=[
            smem(),
            smem(),
            pl.BlockSpec((slabs, block_y * planes, 2 * quarter), lambda g: (0, g, 0)),
            vmem(),
            vmem(),
            vmem(),
            vmem(),
        ],
        out_specs=(
            pl.BlockSpec((2, block_y, quarter, K), lambda g: (0, g, 0, 0)),
            pl.BlockSpec((n_dev, 128), lambda g: (0, 0)),
        ),
        scratch_shapes=[
            pltpu.VMEM((block_y, K), f32),
            pltpu.VMEM((block_y, K), f32),
            pltpu.VMEM((4, quarter, K), f32),
            pltpu.VMEM((quarter, K), f32),
            pltpu.VMEM((quarter, K), f32),
        ]
        + [pltpu.VMEM((8 * quarter, 2 * K), bf16)] * 2
        + [pltpu.VMEM((8 * quarter, 2 * K), f32)] * 2,
        compiler_params=pltpu.CompilerParams(vmem_limit_bytes=60 * 1024 * 1024),
        name="final",
    )(
        jnp.stack([s, a]),
        box,
        moved,
        jnp.asarray(high_z),
        jnp.asarray(low_z),
        jnp.asarray(mod[None, :]),
        jnp.asarray(mod[:, None]),
    )
    return field, spread_totals(sums)


def spread_totals(sums):
    shared = lax.all_to_all(sums, ("slab", "atom"), 0, 0, tiled=True)
    return jnp.sum(shared[:, :7], axis=0)


def plain_final(moved, box, table, a, s, slabs, depth, quarter, norm):
    planes = depth + HALO
    highest = lax.Precision.HIGHEST
    data = moved.reshape(slabs, depth, planes, 2 * quarter)
    own = data[:, :, ABOVE : ABOVE + depth]
    up = jnp.roll(data[:, :, :ABOVE], 1, axis=0)
    down = jnp.roll(data[:, :, ABOVE + depth :], -1, axis=0)
    own = own.at[:, :, :ABOVE].add(up).at[:, :, depth - BELOW :].add(down)
    cosine, sine = (jnp.asarray(t.astype(np.float32)) for t in dft_const())
    flat = jnp.transpose(own, (1, 3, 0, 2)).reshape(depth, 2 * quarter, K)
    real_in, imag_in = flat[:, :quarter], flat[:, quarter:]
    times = functools.partial(jnp.einsum, "yxz,zk->yxk", precision=highest)
    real_part = times(real_in, cosine) + times(imag_in, sine)
    imag_part = times(imag_in, cosine) - times(real_in, sine)
    index_z = jnp.arange(K, dtype=jnp.int32)
    index_y = s * depth + jnp.arange(depth, dtype=jnp.int32)
    index_x = a * quarter + jnp.arange(quarter, dtype=jnp.int32)
    mod = jnp.asarray(moduli_const())

    def folded(index):
        return jnp.where(index < K // 2, index, index - K).astype(f32)

    m_z = (folded(index_z) / box[0])[None, None, :]
    m_y = (folded(index_y) / box[1])[:, None, None]
    m_x = (folded(index_x) / box[2])[None, :, None]
    msq = m_z * m_z + m_y * m_y + m_x * m_x
    anchor = msq == 0.0
    safe = jnp.where(anchor, 1.0, msq)
    volume = box[0] * box[1] * box[2]
    spline_part = mod[index_z][None, None, :] * mod[index_y][:, None, None] * mod[index_x][None, :, None]
    theta = jnp.exp(-math.pi**2 * safe / ewald_beta**2) * spline_part / (math.pi * volume * safe)
    theta = jnp.where(anchor, 0.0, theta)
    half = 0.5 * theta * (real_part * real_part + imag_part * imag_part)
    factor = 2.0 * (1.0 + math.pi**2 * safe / ewald_beta**2) / safe
    terms = [
        half,
        half * (1.0 - factor * m_z * m_z),
        half * (1.0 - factor * m_y * m_y),
        half * (1.0 - factor * m_x * m_x),
        half * (-factor * m_z * m_y),
        half * (-factor * m_z * m_x),
        half * (-factor * m_y * m_x),
    ]
    totals = lax.psum(jnp.stack([jnp.sum(term) for term in terms]), ("slab", "atom")) * norm
    return jnp.stack([theta * real_part, theta * imag_part]), totals


def solution(mesh):
    in_specs = (
        P(None, "slab", "atom"),
        P(None, "slab", "atom"),
        P("slab", "atom"),
        P("slab", "atom"),
        P(),
    )
    out_specs = (P(None, "slab", "atom", None), P())
    return jax.shard_map(body, mesh=mesh, in_specs=in_specs, out_specs=out_specs, check_vma=False)
```
